32 devices in a mesh: ga: 16 (over z, y, x), band: 2 (over core).
Axes of the slice: x: 2, y: 2, z: 4, core: 2. Of those that a mesh axis runs over, the one named last changes fastest.
Arguments:
- psi: bfloat16 [65536, 2048], P('ga', 'band'), may hold values from -1 to 1
- trial: bfloat16 [65536, 256], P('ga', 'band'), may hold values from -1.25 to 1.25
- beta: bfloat16 [65536, 1536], P('ga'), may hold values from -0.0625 to 0.0625
- q_blocks: float32 [128, 18, 18], replicated, may hold values from -6 to 6
- atom_counts: int32 [128], replicated, may hold values from 1 to 18, 1536 in all
Outputs:
- intersection: float32 [2048, 256], P('band', 'ga')
The draws below stay inside these ranges and needn't reach their ends.
Inputs may be any that keep to these rules, and one draw needn't show every extreme that they name: `atom_counts`: the counts sum to 1536; atoms own consecutive projectors in order, and some atom has exactly 18.
All inputs are finite; a program needn't handle non-finite values.
Results may differ from the reference program's by a relative error of at most 0.0003.
Values may be sent and summed in bfloat16 or wider, within the bound.
A program may use at most 64 MiB of HBM per device.

```python
import math
import jax
import jax.numpy as jnp
import numpy as np
from jax import lax

NG = 65536
NB = 2048
BLK = 256
P_SIZE = 1536
NATOM = 128
MAXP = 18


def spiked(drawn, stream_key, source, target, parts, factor):
    def block_of(axis_at):
        return (jnp.arange(drawn.shape[axis_at]) // (drawn.shape[axis_at] // parts)).reshape((-1,) + (1,) * (drawn.ndim - 1 - axis_at))

    first = jax.random.permutation(stream_key, parts)[block_of(target)]
    second = (block_of(target) + parts // 2) % parts
    return jnp.where((block_of(source) == first) | (block_of(source) == second), factor * drawn, drawn)


def levels(own_key, extent, shards, low, high):
    def one(dim, blocks):
        heights = jax.random.uniform(jax.random.fold_in(jax.random.fold_in(own_key, 6), dim), (blocks,), jnp.float32, low / len(shards), high / len(shards))
        return jnp.repeat(jnp.exp(heights), extent[dim] // blocks).reshape((-1,) + (1,) * (len(extent) - dim - 1))

    gain = one(*shards[0])
    for cut in shards[1:]:
        gain = gain * one(*cut)
    return gain


def profile(count, total, most, slope):
    weights = [(1 << 20) // math.isqrt(grade ** slope) + 1 for grade in range(2, count + 1)]
    spare, counts = total - most - (count - 1), [1] * (count - 1)
    while spare > 0:
        candidates = [i for i in range(count - 1) if counts[i] < most]
        mass, remaining = sum([weights[i] for i in candidates]), spare
        for i in candidates:
            addition = min(most - counts[i], max(1, remaining * weights[i] // mass), spare)
            counts[i] = counts[i] + addition
            spare = spare - addition
    return np.array([most] + counts)


def uneven_parts(rng, number_of, total, reach, lean):
    if number_of == 2:
        one = jax.random.randint(rng, (), max(1, total - reach), min(reach, total - 1) + 1)
        return jnp.stack([one, total - one])
    tallies = jnp.asarray(profile(number_of, total, reach, lean), jnp.int32)
    pairs = (number_of - 1) // 2
    donor, taker = tallies[1:1 + 2 * pairs:2], tallies[2:2 + 2 * pairs:2]
    slack = jnp.minimum(donor - 1, reach - taker)
    passed = jax.random.randint(jax.random.fold_in(rng, 1), (pairs,), 0, 1 << 20) % (slack + 1)
    tallies = tallies.at[1:1 + 2 * pairs:2].set(donor - passed).at[2:2 + 2 * pairs:2].set(taker + passed)
    return tallies[jax.random.permutation(jax.random.fold_in(rng, 2), number_of)]


def normal_values(key, dims, width, bound, pieces=(), held_as=jnp.bfloat16):
    values = width * jax.random.normal(key, dims, jnp.float32)
    if pieces:
        values = values * levels(key, dims, pieces, -0.22, 0.18)
    return jnp.clip(values, -bound, bound).astype(held_as)


def bell_draw_with(own_key, shape, scale, limit, pieces, heavy, kind=jnp.bfloat16):
    drawn = scale * jax.random.normal(own_key, shape, jnp.float32)
    if pieces:
        drawn = drawn * levels(own_key, shape, pieces, -0.22, 0.18)
    return jnp.clip(spiked(drawn, jax.random.fold_in(own_key, 3), *heavy), -limit, limit).astype(kind)


def setup_inputs(seed: int = 0) -> dict:
    seeds = jax.random.split(jax.random.key(seed), 6)
    return {
        "psi": normal_values(seeds[0], (NG, NB), (NG ** -0.25), 1.0, ((0, 16), (1, 2))),
        "trial": bell_draw_with(seeds[1], (NG, BLK), (NG ** -0.25), 1.25, ((0, 16), (1, 2)), (0, 1, 16, 2.0)),
        "beta": normal_values(seeds[2], (NG, P_SIZE), ((P_SIZE * MAXP * NG) ** -0.25), 0.0625, ((0, 16),)),
        "q_blocks": normal_values(seeds[3], (NATOM, MAXP, MAXP), 1.0, 6.0, (), jnp.float32),
        "atom_counts": uneven_parts(seeds[4], NATOM, P_SIZE, MAXP, 1).astype(jnp.int32),
    }


def contract(left, right, precision=None):
    return lax.dot_general(left, right, (((0,), (0,)), ((), ())), precision=precision, preferred_element_type=jnp.float32)


def reference(psi, trial, beta, q_blocks, atom_counts):
    offsets = jnp.cumsum(atom_counts, dtype=jnp.int32) - atom_counts
    ids = jnp.arange(P_SIZE, dtype=jnp.int32)
    below = offsets[None, :] <= ids[:, None]
    atom_ids = jnp.sum(below.astype(jnp.int32), axis=1, dtype=jnp.int32) - 1
    starts = jnp.max(jnp.where(below, offsets[None, :], 0), axis=1)
    position = ids - starts
    same_atom = atom_ids[:, None] == atom_ids[None, :]
    entries = q_blocks[atom_ids[:, None], position[:, None], position[None, :]]
    q_matrix = jnp.where(same_atom, entries, jnp.zeros_like(entries))
    proj_bands = contract(beta, psi)
    proj_trial = contract(beta, trial)
    weighted = jnp.dot(q_matrix, proj_trial, precision=lax.Precision.HIGHEST, preferred_element_type=jnp.float32)
    plain = contract(psi, trial)
    return plain + contract(proj_bands, weighted, lax.Precision.HIGHEST)
```

```python
import functools

import jax
import jax.numpy as jnp
from jax import lax
from jax.experimental import pallas as pl
from jax.experimental.pallas import tpu as pltpu
from jax.sharding import PartitionSpec as P

MESH = pl.DeviceIdType.MESH
precise = lax.Precision.HIGHEST
F32, BF16 = jnp.float32, jnp.bfloat16


def contract(left, right, precision=None):
    return lax.dot_general(
        left, right, (((0,), (0,)), ((), ())), precision=precision, preferred_element_type=F32
    )


def split2(x):
    hi = x.astype(BF16)
    return hi, (x - hi.astype(F32)).astype(BF16)


def kernel(
    n, maxp, psi_h, trial_h, beta_h, q_ref, cnt_ref, out_ref,
    psi_v, beta_v, trial_v, trial_t, q_parts, qd, proj, rs1, wall, whl, s_buf, fin, rs2,
    trial_sem, beta_sem, psi_sem, send1, recv1, send2, recv2, xs, xr, send3, recv3,
):
    me = lax.axis_index("ga")
    band = lax.axis_index("band")
    g, cols = trial_v.shape
    p_size = beta_v.shape[1]
    nbands = psi_v.shape[1]
    natom = cnt_ref.shape[1]
    mp = q_ref.shape[0] // maxp
    r1 = cols // n
    r2 = out_ref.shape[0]
    beta_chunks = beta_sem.shape[0]
    bw = p_size // beta_chunks
    psi_chunks = psi_sem.shape[0]
    pw = nbands // psi_chunks
    s_chunks = xs.shape[0]
    sw = g // s_chunks

    def aligned(i, size):
        return pl.ds(pl.multiple_of(i * size, size), size)

    def beta_copy(c):
        at = (slice(None), pl.ds(c * bw, bw))
        return pltpu.make_async_copy(beta_h.at[at], beta_v.at[at], beta_sem.at[c])

    def psi_copy(c):
        at = (slice(None), pl.ds(c * pw, pw))
        return pltpu.make_async_copy(psi_h.at[at], psi_v.at[at], psi_sem.at[c])

    trial_copy = pltpu.make_async_copy(trial_h, trial_v, trial_sem)
    trial_copy.start()
    for c in range(beta_chunks):
        beta_copy(c).start()
    for c in range(psi_chunks):
        psi_copy(c).start()

    barrier = pltpu.get_barrier_semaphore()

    def greet(d, _):
        pl.semaphore_signal(
            barrier, inc=1, device_id=(lax.rem(me + d, n), band), device_id_type=MESH
        )
        return 0

    lax.fori_loop(1, n, greet, 0)
    pl.semaphore_signal(barrier, inc=1, device_id=(me, 1 - band), device_id_type=MESH)

    cnt = cnt_ref[...].astype(F32)
    row = lax.broadcasted_iota(jnp.int32, (natom, natom), 0)
    col = lax.broadcasted_iota(jnp.int32, (natom, natom), 1)
    offs = jnp.sum(jnp.where(col < row, cnt, 0.0), axis=1, keepdims=True)
    own = jnp.sum(jnp.where(col == row, cnt, 0.0), axis=1, keepdims=True)
    q = q_ref[...]
    q_hi = q.astype(BF16)
    rest = q - q_hi.astype(F32)
    q_mid = rest.astype(BF16)
    q_parts[0] = q_hi
    q_parts[1] = q_mid
    q_parts[2] = (rest - q_mid.astype(F32)).astype(BF16)
    lanes = 256
    nd = qd.shape[0]

    def diagonals(c, _):
        ids = (c * lanes + lax.broadcasted_iota(jnp.int32, (natom, lanes), 1)).astype(F32)
        owns = (offs <= ids) & (ids < offs + own)
        pos = jnp.sum(jnp.where(owns, ids - offs, 0.0), axis=0, keepdims=True)
        count = jnp.sum(jnp.where(owns, jnp.broadcast_to(own, owns.shape), 0.0), axis=0, keepdims=True)
        pick = jnp.where(owns, 1.0, 0.0).astype(BF16)
        flat = jnp.dot(q_parts[0], pick, preferred_element_type=F32)
        flat += jnp.dot(q_parts[1], pick, preferred_element_type=F32)
        flat += jnp.dot(q_parts[2], pick, preferred_element_type=F32)
        q_row = jnp.zeros((mp, lanes), F32)
        for i in range(maxp):
            q_row += jnp.where(pos == float(i), flat[i * mp : (i + 1) * mp], 0.0)
        at = pos + lax.broadcasted_iota(jnp.int32, (nd, lanes), 0).astype(F32) - float(maxp - 1)
        entries = jnp.zeros((nd, lanes), F32)
        for j in range(maxp):
            entries += jnp.where(at == float(j), q_row[j : j + 1], 0.0)
        qd[:, aligned(c, lanes)] = jnp.where(at < count, entries, 0.0)
        return 0

    lax.fori_loop(0, p_size // lanes, diagonals, 0)

    trial_copy.wait()

    def turn(k, _):
        trial_t[:, aligned(k, sw)] = trial_v[aligned(k, sw), :].T
        return 0

    lax.fori_loop(0, s_chunks, turn, 0)

    pl.semaphore_wait(barrier, n)

    def scatter1(c, d):
        peer = lax.rem(me + d, n)
        at = pl.ds(c * bw, bw)
        return pltpu.make_async_remote_copy(
            src_ref=proj.at[aligned(peer, r1), at],
            dst_ref=rs1.at[d, :, at],
            send_sem=send1.at[c, d],
            recv_sem=recv1.at[c, d],
            device_id=(peer, band),
            device_id_type=MESH,
        )

    for c in range(beta_chunks):
        beta_copy(c).wait()
        at = pl.ds(c * bw, bw)
        proj[:, at] = jnp.dot(trial_t[...], beta_v[:, at], preferred_element_type=F32)

        def start1(d, _, c=c):
            scatter1(c, d).start()
            return 0

        lax.fori_loop(1, n, start1, 0)

    for c in range(beta_chunks):

        def wait1(d, _, c=c):
            scatter1(c, d).wait()
            return 0

        lax.fori_loop(1, n, wait1, 0)

    def add1(d, total):
        return total + rs1[d]

    x = lax.fori_loop(1, n, add1, proj[aligned(me, r1), :])
    acc = jnp.zeros_like(x)
    for d in range(2 * maxp - 1):
        shift = (maxp - 1 - d) % p_size
        moved = x if shift == 0 else pltpu.roll(x, shift, axis=1)
        acc += qd[d : d + 1, :] * moved
    wall[aligned(me, r1), :] = acc

    def gather(d):
        peer = lax.rem(me + d, n)
        return pltpu.make_async_remote_copy(
            src_ref=wall.at[aligned(me, r1), :],
            dst_ref=wall.at[aligned(me, r1), :],
            send_sem=send2.at[d],
            recv_sem=recv2.at[d],
            device_id=(peer, band),
            device_id_type=MESH,
        )

    def start2(d, _):
        gather(d).start()
        return 0

    def wait2(d, _):
        gather(d).wait()
        return 0

    lax.fori_loop(1, n, start2, 0)
    lax.fori_loop(1, n, wait2, 0)
    hi, lo = split2(wall[...])
    whl[:cols, :] = hi
    whl[cols:, :] = lo

    base = band * (2 * cols)

    def exchange(k):
        at = (pl.ds(pl.multiple_of(base, 2 * cols), 2 * cols), aligned(k, sw))
        return pltpu.make_async_remote_copy(
            src_ref=s_buf.at[at],
            dst_ref=s_buf.at[at],
            send_sem=xs.at[k],
            recv_sem=xr.at[k],
            device_id=(me, 1 - band),
            device_id_type=MESH,
        )

    def lift(k, _):
        both = lax.dot_general(
            whl[...], beta_v[aligned(k, sw), :], (((1,), (1,)), ((), ())), preferred_element_type=F32
        )
        s = both[:cols] + both[cols:] + trial_t[:, aligned(k, sw)].astype(F32)
        s_hi, s_lo = split2(s)
        s_buf[pl.ds(pl.multiple_of(base, 2 * cols), cols), aligned(k, sw)] = s_hi
        s_buf[pl.ds(pl.multiple_of(base + cols, cols), cols), aligned(k, sw)] = s_lo
        exchange(k).start()
        return 0

    lax.fori_loop(0, s_chunks, lift, 0)

    def wait_x(k, _):
        exchange(k).wait()
        return 0

    lax.fori_loop(0, s_chunks, wait_x, 0)

    def scatter3(c, d):
        peer = lax.rem(me + d, n)
        return pltpu.make_async_remote_copy(
            src_ref=fin.at[aligned(peer, r2), aligned(c, pw)],
            dst_ref=rs2.at[d, :, aligned(c, pw)],
            send_sem=send3.at[c, d],
            recv_sem=recv3.at[c, d],
            device_id=(peer, band),
            device_id_type=MESH,
        )

    for c in range(psi_chunks):
        psi_copy(c).wait()

    def share(c, _):
        f = jnp.dot(s_buf[...], psi_v[:, aligned(c, pw)], preferred_element_type=F32)
        for b in range(2):
            at = 2 * b * cols
            fin[b * cols : (b + 1) * cols, aligned(c, pw)] = (
                f[at : at + cols] + f[at + cols : at + 2 * cols]
            )

        def start3(d, _):
            scatter3(c, d).start()
            return 0

        lax.fori_loop(1, n, start3, 0)
        return 0

    lax.fori_loop(0, psi_chunks, share, 0)

    def finish(c, _):
        def wait3(d, total):
            scatter3(c, d).wait()
            return total + rs2[d, :, aligned(c, pw)]

        out_ref[:, aligned(c, pw)] = lax.fori_loop(
            1, n, wait3, fin[aligned(me, r2), aligned(c, pw)]
        )
        return 0

    lax.fori_loop(0, psi_chunks, finish, 0)


def fused(n, blk, psi, trial, beta, q_blocks, atom_counts):
    g, cols = trial.shape
    nbands = psi.shape[1]
    p_size = beta.shape[1]
    natom, maxp = q_blocks.shape[:2]
    mp = -(-maxp // 8) * 8
    nd = -(-(2 * maxp - 1) // 8) * 8
    r1, r2 = cols // n, blk // n
    beta_chunks, psi_chunks, s_chunks = 3, 4, 8
    q_flat = jnp.pad(q_blocks, ((0, 0), (0, 0), (0, mp - maxp)))
    q_flat = q_flat.transpose(1, 2, 0).reshape(maxp * mp, natom)
    dma = pltpu.SemaphoreType.DMA
    out = pl.pallas_call(
        functools.partial(kernel, n, maxp),
        out_shape=jax.ShapeDtypeStruct((r2, nbands), F32),
        in_specs=[pl.BlockSpec(memory_space=pl.ANY)] * 3
        + [pl.BlockSpec(memory_space=pltpu.VMEM)] * 2,
        out_specs=pl.BlockSpec(memory_space=pltpu.VMEM),
        scratch_shapes=[
            pltpu.VMEM((g, nbands), BF16),
            pltpu.VMEM((g, p_size), BF16),
            pltpu.VMEM((g, cols), BF16),
            pltpu.VMEM((cols, g), BF16),
            pltpu.VMEM((3, maxp * mp, natom), BF16),
            pltpu.VMEM((nd, p_size), F32),
            pltpu.VMEM((cols, p_size), F32),
            pltpu.VMEM((n, r1, p_size), F32),
            pltpu.VMEM((cols, p_size), F32),
            pltpu.VMEM((2 * cols, p_size), BF16),
            pltpu.VMEM((4 * cols, g), BF16),
            pltpu.VMEM((2 * cols, nbands), F32),
            pltpu.VMEM((n, r2, nbands), F32),
            dma,
            dma((beta_chunks,)),
            dma((psi_chunks,)),
            dma((beta_chunks, n)),
            dma((beta_chunks, n)),
            dma((n,)),
            dma((n,)),
            dma((s_chunks,)),
            dma((s_chunks,)),
            dma((psi_chunks, n)),
            dma((psi_chunks, n)),
        ],
        compiler_params=pltpu.CompilerParams(
            collective_id=0, has_side_effects=True, vmem_limit_bytes=60 * 1024 * 1024
        ),
    )(psi, trial, beta, q_flat, atom_counts.reshape(1, natom))
    return out.T


def q_dense(atom_counts, q_blocks, p_size):
    offsets = jnp.cumsum(atom_counts, dtype=jnp.int32) - atom_counts
    natom, maxp = q_blocks.shape[:2]
    ids = jnp.arange(p_size, dtype=jnp.int32)
    owns = (offsets[None, :] <= ids[:, None]) & (ids[:, None] < (offsets + atom_counts)[None, :])
    pos = jnp.sum(jnp.where(owns, ids[:, None] - offsets[None, :], 0), axis=1)
    atom = jnp.sum(jnp.where(owns, jnp.arange(natom, dtype=jnp.int32)[None, :], 0), axis=1)
    flat = jnp.dot(owns.astype(F32), q_blocks.reshape(natom, maxp * maxp), precision=precise)
    place = pos[:, None] == jnp.arange(maxp, dtype=jnp.int32)[None, :]
    rows = jnp.sum(jnp.where(place[:, :, None], flat.reshape(p_size, maxp, maxp), 0.0), axis=1)
    entries = jnp.dot(rows, place.astype(F32).T, precision=precise)
    return jnp.where(atom[:, None] == atom[None, :], entries, 0.0)


def general(psi, trial, beta, q_blocks, atom_counts):
    own = lax.psum(contract(beta, trial), "ga")
    weighted = jnp.dot(q_dense(atom_counts, q_blocks, beta.shape[1]), own, precision=precise)
    w_hi, w_lo = split2(weighted)
    both = jnp.dot(beta, jnp.concatenate([w_hi, w_lo], axis=1), preferred_element_type=F32)
    cols = trial.shape[1]
    s = both[:, :cols] + both[:, cols:] + trial.astype(F32)
    s_hi, s_lo = split2(lax.all_gather(s, "band", axis=1, tiled=True))
    part = contract(psi, s_hi) + contract(psi, s_lo)
    return lax.psum_scatter(part, "ga", scatter_dimension=1, tiled=True)


def solution(mesh):
    n, bands = mesh.shape["ga"], mesh.shape["band"]

    def shards(psi, trial, beta, q_blocks, atom_counts):
        g, cols = trial.shape
        blk = cols * bands
        fits = (
            bands == 2
            and cols % 128 == 0
            and cols % (8 * n) == 0
            and blk % (8 * n) == 0
            and g % 4096 == 0
            and beta.shape[1] % 768 == 0
            and psi.shape[1] % 512 == 0
            and q_blocks.shape[0] % 128 == 0
        )
        if fits:
            return fused(n, blk, psi, trial, beta, q_blocks, atom_counts)
        return general(psi, trial, beta, q_blocks, atom_counts)

    in_specs = (P("ga", "band"), P("ga", "band"), P("ga", None), P(), P())
    out_specs = P("band", "ga")
    return jax.shard_map(shards, mesh=mesh, in_specs=in_specs, out_specs=out_specs, check_vma=False)
```

```python
import functools

import jax
import jax.numpy as jnp
from jax import lax
from jax.experimental import pallas as pl
from jax.experimental.pallas import tpu as pltpu
from jax.sharding import PartitionSpec as P

MESH = pl.DeviceIdType.MESH
precise = lax.Precision.HIGHEST
F32, BF16 = jnp.float32, jnp.bfloat16


def contract(left, right, precision=None):
    return lax.dot_general(
        left, right, (((0,), (0,)), ((), ())), precision=precision, preferred_element_type=F32
    )


def split2(x):
    hi = x.astype(BF16)
    return hi, (x - hi.astype(F32)).astype(BF16)


def kernel(
    n, inner, maxp, psi_h, trial_h, beta_h, q_ref, cnt_ref, out_ref,
    psi_v, beta_v, trial_v, trial_t, q_parts, qd, proj, in1, mid1, end1, wall, whl, s_buf,
    fin, in3, mid3, end3, trial_sem, beta_sem, psi_sem, send1, recv1, send1b, recv1b,
    send2, recv2, send2b, recv2b, xs, xr, send3, recv3, send3b, recv3b,
):
    me = lax.axis_index("ga")
    band = lax.axis_index("band")
    outer = n // inner
    w, z = lax.rem(me, inner), lax.div(me, inner)

    def mate(d):
        return lax.rem(w + d, inner)

    def far(e):
        return lax.rem(z + e, outer)

    def reach(to_z, to_w):
        return dict(device_id=(to_z * inner + to_w, band), device_id_type=MESH)

    g, cols = trial_v.shape
    p_size = beta_v.shape[1]
    nbands = psi_v.shape[1]
    natom = cnt_ref.shape[1]
    mp = q_ref.shape[0] // maxp
    r1 = cols // n
    r2 = out_ref.shape[0]
    beta_chunks = beta_sem.shape[0]
    bw = p_size // beta_chunks
    psi_chunks = psi_sem.shape[0]
    pw = nbands // psi_chunks
    s_chunks = xs.shape[0]
    sw = g // s_chunks

    def aligned(i, size):
        return pl.ds(i * size if isinstance(i, int) else pl.multiple_of(i * size, size), size)

    def beta_copy(c):
        at = (slice(None), pl.ds(c * bw, bw))
        return pltpu.make_async_copy(beta_h.at[at], beta_v.at[at], beta_sem.at[c])

    def psi_copy(c):
        at = (slice(None), pl.ds(c * pw, pw))
        return pltpu.make_async_copy(psi_h.at[at], psi_v.at[at], psi_sem.at[c])

    trial_copy = pltpu.make_async_copy(trial_h, trial_v, trial_sem)
    trial_copy.start()
    for c in range(beta_chunks):
        beta_copy(c).start()
    for c in range(psi_chunks):
        psi_copy(c).start()

    barrier = pltpu.get_barrier_semaphore()

    for d in range(1, inner):
        pl.semaphore_signal(barrier, inc=1, **reach(z, mate(d)))
    for e in range(1, outer):
        pl.semaphore_signal(barrier, inc=1, **reach(far(e), w))
    pl.semaphore_signal(barrier, inc=1, device_id=(me, 1 - band), device_id_type=MESH)

    cnt = cnt_ref[...].astype(F32)
    row = lax.broadcasted_iota(jnp.int32, (natom, natom), 0)
    col = lax.broadcasted_iota(jnp.int32, (natom, natom), 1)
    offs = jnp.sum(jnp.where(col < row, cnt, 0.0), axis=1, keepdims=True)
    own = jnp.sum(jnp.where(col == row, cnt, 0.0), axis=1, keepdims=True)
    q = q_ref[...]
    q_hi = q.astype(BF16)
    rest = q - q_hi.astype(F32)
    q_mid = rest.astype(BF16)
    q_parts[0] = q_hi
    q_parts[1] = q_mid
    q_parts[2] = (rest - q_mid.astype(F32)).astype(BF16)
    lanes = 256
    nd = qd.shape[0]

    def diagonals(c, _):
        ids = (c * lanes + lax.broadcasted_iota(jnp.int32, (natom, lanes), 1)).astype(F32)
        owns = (offs <= ids) & (ids < offs + own)
        pos = jnp.sum(jnp.where(owns, ids - offs, 0.0), axis=0, keepdims=True)
        count = jnp.sum(jnp.where(owns, jnp.broadcast_to(own, owns.shape), 0.0), axis=0, keepdims=True)
        pick = jnp.where(owns, 1.0, 0.0).astype(BF16)
        flat = jnp.dot(q_parts[0], pick, preferred_element_type=F32)
        flat += jnp.dot(q_parts[1], pick, preferred_element_type=F32)
        flat += jnp.dot(q_parts[2], pick, preferred_element_type=F32)
        q_row = jnp.zeros((mp, lanes), F32)
        for i in range(maxp):
            q_row += jnp.where(pos == float(i), flat[i * mp : (i + 1) * mp], 0.0)
        at = pos + lax.broadcasted_iota(jnp.int32, (nd, lanes), 0).astype(F32) - float(maxp - 1)
        entries = jnp.zeros((nd, lanes), F32)
        for j in range(maxp):
            entries += jnp.where(at == float(j), q_row[j : j + 1], 0.0)
        qd[:, aligned(c, lanes)] = jnp.where(at < count, entries, 0.0)
        return 0

    lax.fori_loop(0, p_size // lanes, diagonals, 0)

    trial_copy.wait()

    def turn(k, _):
        trial_t[:, aligned(k, sw)] = trial_v[aligned(k, sw), :].T
        return 0

    lax.fori_loop(0, s_chunks, turn, 0)

    pl.semaphore_wait(barrier, inner + outer - 1)

    def inner1(c, d):
        at = pl.ds(c * bw, bw)
        return pltpu.make_async_remote_copy(
            src_ref=proj.at[aligned(mate(d), outer * r1), at],
            dst_ref=in1.at[d, :, at],
            send_sem=send1.at[c, d],
            recv_sem=recv1.at[c, d],
            **reach(z, mate(d)),
        )

    def outer1(c, e):
        at = pl.ds(c * bw, bw)
        return pltpu.make_async_remote_copy(
            src_ref=mid1.at[aligned(far(e), r1), at],
            dst_ref=end1.at[e, :, at],
            send_sem=send1b.at[c, e],
            recv_sem=recv1b.at[c, e],
            **reach(far(e), w),
        )

    def middle1(c):
        at = pl.ds(c * bw, bw)
        total = proj[aligned(w, outer * r1), at]
        for d in range(1, inner):
            inner1(c, d).wait()
            total += in1[d, :, at]
        mid1[:, at] = total
        for e in range(1, outer):
            outer1(c, e).start()

    for c in range(beta_chunks):
        beta_copy(c).wait()
        at = pl.ds(c * bw, bw)
        proj[:, at] = jnp.dot(trial_t[...], beta_v[:, at], preferred_element_type=F32)
        for d in range(1, inner):
            inner1(c, d).start()
        if c:
            middle1(c - 1)
    middle1(beta_chunks - 1)

    for c in range(beta_chunks):
        for e in range(1, outer):
            outer1(c, e).wait()
    x = mid1[aligned(z, r1), :]
    for e in range(1, outer):
        x += end1[e]
    acc = jnp.zeros_like(x)
    for d in range(2 * maxp - 1):
        shift = (maxp - 1 - d) % p_size
        moved = x if shift == 0 else pltpu.roll(x, shift, axis=1)
        acc += qd[d : d + 1, :] * moved
    mine = w * outer + z
    wall[aligned(mine, r1), :] = acc

    def outer2(e):
        return pltpu.make_async_remote_copy(
            src_ref=wall.at[aligned(mine, r1), :],
            dst_ref=wall.at[aligned(mine, r1), :],
            send_sem=send2.at[e],
            recv_sem=recv2.at[e],
            **reach(far(e), w),
        )

    def inner2(e, d):
        block = w * outer + lax.rem(z + outer - e, outer)
        return pltpu.make_async_remote_copy(
            src_ref=wall.at[aligned(block, r1), :],
            dst_ref=wall.at[aligned(block, r1), :],
            send_sem=send2b.at[e, d],
            recv_sem=recv2b.at[e, d],
            **reach(z, mate(d)),
        )

    for e in range(1, outer):
        outer2(e).start()
    for e in range(outer):
        if e:
            outer2(e).wait()
        for d in range(1, inner):
            inner2(e, d).start()
    for e in range(outer):
        for d in range(1, inner):
            inner2(e, d).wait()
    hi, lo = split2(wall[...])
    whl[:cols, :] = hi
    whl[cols:, :] = lo

    base = band * (2 * cols)

    def exchange(k):
        at = (pl.ds(pl.multiple_of(base, 2 * cols), 2 * cols), aligned(k, sw))
        return pltpu.make_async_remote_copy(
            src_ref=s_buf.at[at],
            dst_ref=s_buf.at[at],
            send_sem=xs.at[k],
            recv_sem=xr.at[k],
            device_id=(me, 1 - band),
            device_id_type=MESH,
        )

    def lift(k, _):
        both = lax.dot_general(
            whl[...], beta_v[aligned(k, sw), :], (((1,), (1,)), ((), ())), preferred_element_type=F32
        )
        s = both[:cols] + both[cols:] + trial_t[:, aligned(k, sw)].astype(F32)
        s_hi, s_lo = split2(s)
        s_buf[pl.ds(pl.multiple_of(base, 2 * cols), cols), aligned(k, sw)] = s_hi
        s_buf[pl.ds(pl.multiple_of(base + cols, cols), cols), aligned(k, sw)] = s_lo
        exchange(k).start()
        return 0

    lax.fori_loop(0, s_chunks, lift, 0)

    def wait_x(k, _):
        exchange(k).wait()
        return 0

    lax.fori_loop(0, s_chunks, wait_x, 0)

    def inner3(c, d):
        return pltpu.make_async_remote_copy(
            src_ref=fin.at[:, mate(d), :, aligned(c, pw)],
            dst_ref=in3.at[d, :, :, aligned(c, pw)],
            send_sem=send3.at[c, d],
            recv_sem=recv3.at[c, d],
            **reach(z, mate(d)),
        )

    def outer3(c, e):
        return pltpu.make_async_remote_copy(
            src_ref=mid3.at[far(e), :, aligned(c, pw)],
            dst_ref=end3.at[e, :, aligned(c, pw)],
            send_sem=send3b.at[c, e],
            recv_sem=recv3b.at[c, e],
            **reach(far(e), w),
        )

    def middle3(c):
        for d in range(1, inner):
            inner3(c, d).wait()
        for to in range(outer):
            total = fin[to, w, :, aligned(c, pw)]
            for d in range(1, inner):
                total += in3[d, to, :, aligned(c, pw)]
            mid3[to, :, aligned(c, pw)] = total
        for e in range(1, outer):
            outer3(c, e).start()

    for c in range(psi_chunks):
        psi_copy(c).wait()

    def share(c):
        f = jnp.dot(s_buf[...], psi_v[:, aligned(c, pw)], preferred_element_type=F32)
        for b in range(2):
            at = 2 * b * cols
            whole = f[at : at + cols] + f[at + cols : at + 2 * cols]
            fin[b * half : (b + 1) * half, :, :, aligned(c, pw)] = whole.reshape(
                half, inner, r2, pw
            )
        for d in range(1, inner):
            inner3(c, d).start()

    half = outer // 2
    for c in range(psi_chunks):
        share(c)
        if c:
            middle3(c - 1)
    middle3(psi_chunks - 1)

    for c in range(psi_chunks):
        total = mid3[z, :, aligned(c, pw)]
        for e in range(1, outer):
            outer3(c, e).wait()
            total += end3[e, :, aligned(c, pw)]
        out_ref[:, aligned(c, pw)] = total


def fused(n, inner, blk, psi, trial, beta, q_blocks, atom_counts):
    g, cols = trial.shape
    nbands = psi.shape[1]
    p_size = beta.shape[1]
    natom, maxp = q_blocks.shape[:2]
    mp = -(-maxp // 8) * 8
    nd = -(-(2 * maxp - 1) // 8) * 8
    r1, r2 = cols // n, blk // n
    outer = n // inner
    beta_chunks, psi_chunks, s_chunks = 3, 4, 8
    q_flat = jnp.pad(q_blocks, ((0, 0), (0, 0), (0, mp - maxp)))
    q_flat = q_flat.transpose(1, 2, 0).reshape(maxp * mp, natom)
    dma = pltpu.SemaphoreType.DMA
    out = pl.pallas_call(
        functools.partial(kernel, n, inner, maxp),
        out_shape=jax.ShapeDtypeStruct((r2, nbands), F32),
        in_specs=[pl.BlockSpec(memory_space=pl.ANY)] * 3
        + [pl.BlockSpec(memory_space=pltpu.VMEM)] * 2,
        out_specs=pl.BlockSpec(memory_space=pltpu.VMEM),
        scratch_shapes=[
            pltpu.VMEM((g, nbands), BF16),
            pltpu.VMEM((g, p_size), BF16),
            pltpu.VMEM((g, cols), BF16),
            pltpu.VMEM((cols, g), BF16),
            pltpu.VMEM((3, maxp * mp, natom), BF16),
            pltpu.VMEM((nd, p_size), F32),
            pltpu.VMEM((cols, p_size), F32),
            pltpu.VMEM((inner, outer * r1, p_size), F32),
            pltpu.VMEM((outer * r1, p_size), F32),
            pltpu.VMEM((outer, r1, p_size), F32),
            pltpu.VMEM((cols, p_size), F32),
            pltpu.VMEM((2 * cols, p_size), BF16),
            pltpu.VMEM((4 * cols, g), BF16),
            pltpu.VMEM((outer, inner, r2, nbands), F32),
            pltpu.VMEM((inner, outer, r2, nbands), F32),
            pltpu.VMEM((outer, r2, nbands), F32),
            pltpu.VMEM((outer, r2, nbands), F32),
            dma,
            dma((beta_chunks,)),
            dma((psi_chunks,)),
            dma((beta_chunks, inner)),
            dma((beta_chunks, inner)),
            dma((beta_chunks, outer)),
            dma((beta_chunks, outer)),
            dma((outer,)),
            dma((outer,)),
            dma((outer, inner)),
            dma((outer, inner)),
            dma((s_chunks,)),
            dma((s_chunks,)),
            dma((psi_chunks, inner)),
            dma((psi_chunks, inner)),
            dma((psi_chunks, outer)),
            dma((psi_chunks, outer)),
        ],
        compiler_params=pltpu.CompilerParams(
            collective_id=0, has_side_effects=True, vmem_limit_bytes=60 * 1024 * 1024
        ),
    )(psi, trial, beta, q_flat, atom_counts.reshape(1, natom))
    return out.T


def q_dense(atom_counts, q_blocks, p_size):
    offsets = jnp.cumsum(atom_counts, dtype=jnp.int32) - atom_counts
    natom, maxp = q_blocks.shape[:2]
    ids = jnp.arange(p_size, dtype=jnp.int32)
    owns = (offsets[None, :] <= ids[:, None]) & (ids[:, None] < (offsets + atom_counts)[None, :])
    pos = jnp.sum(jnp.where(owns, ids[:, None] - offsets[None, :], 0), axis=1)
    atom = jnp.sum(jnp.where(owns, jnp.arange(natom, dtype=jnp.int32)[None, :], 0), axis=1)
    flat = jnp.dot(owns.astype(F32), q_blocks.reshape(natom, maxp * maxp), precision=precise)
    place = pos[:, None] == jnp.arange(maxp, dtype=jnp.int32)[None, :]
    rows = jnp.sum(jnp.where(place[:, :, None], flat.reshape(p_size, maxp, maxp), 0.0), axis=1)
    entries = jnp.dot(rows, place.astype(F32).T, precision=precise)
    return jnp.where(atom[:, None] == atom[None, :], entries, 0.0)


def general(psi, trial, beta, q_blocks, atom_counts):
    own = lax.psum(contract(beta, trial), "ga")
    weighted = jnp.dot(q_dense(atom_counts, q_blocks, beta.shape[1]), own, precision=precise)
    w_hi, w_lo = split2(weighted)
    both = jnp.dot(beta, jnp.concatenate([w_hi, w_lo], axis=1), preferred_element_type=F32)
    cols = trial.shape[1]
    s = both[:, :cols] + both[:, cols:] + trial.astype(F32)
    s_hi, s_lo = split2(lax.all_gather(s, "band", axis=1, tiled=True))
    part = contract(psi, s_hi) + contract(psi, s_lo)
    return lax.psum_scatter(part, "ga", scatter_dimension=1, tiled=True)


def solution(mesh):
    n, bands = mesh.shape["ga"], mesh.shape["band"]
    inner = 4

    def shards(psi, trial, beta, q_blocks, atom_counts):
        g, cols = trial.shape
        blk = cols * bands
        fits = (
            bands == 2
            and n % (2 * inner) == 0
            and cols % 128 == 0
            and cols % (8 * n) == 0
            and blk % (8 * n) == 0
            and g % 4096 == 0
            and beta.shape[1] % 768 == 0
            and psi.shape[1] % 512 == 0
            and q_blocks.shape[0] % 128 == 0
        )
        if fits:
            return fused(n, inner, blk, psi, trial, beta, q_blocks, atom_counts)
        return general(psi, trial, beta, q_blocks, atom_counts)

    in_specs = (P("ga", "band"), P("ga", "band"), P("ga", None), P(), P())
    out_specs = P("band", "ga")
    return jax.shard_map(shards, mesh=mesh, in_specs=in_specs, out_specs=out_specs, check_vma=False)
```

```python
import functools

import jax
import jax.numpy as jnp
from jax import lax
from jax.experimental import pallas as pl
from jax.experimental.pallas import tpu as pltpu
from jax.sharding import PartitionSpec as P

MESH = pl.DeviceIdType.MESH
precise = lax.Precision.HIGHEST
F32, BF16 = jnp.float32, jnp.bfloat16


def contract(left, right, precision=None):
    return lax.dot_general(
        left, right, (((0,), (0,)), ((), ())), precision=precision, preferred_element_type=F32
    )


def split2(x):
    hi = x.astype(BF16)
    return hi, (x - hi.astype(F32)).astype(BF16)


def kernel(
    n, inner, maxp, psi_h, trial_h, beta_h, q_ref, cnt_ref, out_ref,
    psi_v, beta_v, trial_v, trial_t, q_parts, qd, proj, in1, mid1, end1, wall, whl, s_buf,
    fin, in3, mid3, end3, trial_sem, beta_sem, psi_sem, send1, recv1, send1b, recv1b,
    send2, recv2, send2b, recv2b, xs, xr, send3, recv3, send3b, recv3b,
):
    me = lax.axis_index("ga")
    band = lax.axis_index("band")
    outer = n // inner
    w, z = lax.rem(me, inner), lax.div(me, inner)

    flip, cross = w + 1 - 2 * lax.rem(w, 2), lax.rem(w + 2, 4)
    via = (1 - band) * flip + band * cross
    last = band * flip + (1 - band) * cross
    hop = {1: via, 2: last, 3: via}
    meant = {1: via, 2: last, 3: 3 - w}

    def far(e):
        return lax.rem(z + e, outer)

    def reach(to_z, to_w):
        return dict(device_id=(to_z * inner + to_w, band), device_id_type=MESH)

    g, cols = trial_v.shape
    p_size = beta_v.shape[1]
    nbands = psi_v.shape[1]
    natom = cnt_ref.shape[1]
    mp = q_ref.shape[0] // maxp
    r1 = cols // n
    r2 = out_ref.shape[0]
    beta_chunks = beta_sem.shape[0]
    bw = p_size // beta_chunks
    psi_chunks = psi_sem.shape[0]
    pw = nbands // psi_chunks
    s_chunks = xs.shape[0]
    sw = g // s_chunks

    def aligned(i, size):
        return pl.ds(i * size if isinstance(i, int) else pl.multiple_of(i * size, size), size)

    def beta_copy(c):
        at = (slice(None), pl.ds(c * bw, bw))
        return pltpu.make_async_copy(beta_h.at[at], beta_v.at[at], beta_sem.at[c])

    def psi_copy(c):
        at = (slice(None), pl.ds(c * pw, pw))
        return pltpu.make_async_copy(psi_h.at[at], psi_v.at[at], psi_sem.at[c])

    trial_copy = pltpu.make_async_copy(trial_h, trial_v, trial_sem)
    trial_copy.start()
    for c in range(beta_chunks):
        beta_copy(c).start()
    for c in range(psi_chunks):
        psi_copy(c).start()

    barrier = pltpu.get_barrier_semaphore()

    for d in range(2):
        pl.semaphore_signal(barrier, inc=1, **reach(z, (via, last)[d]))
    for e in range(1, outer):
        pl.semaphore_signal(barrier, inc=1, **reach(far(e), w))
    pl.semaphore_signal(barrier, inc=1, device_id=(me, 1 - band), device_id_type=MESH)

    cnt = cnt_ref[...].astype(F32)
    row = lax.broadcasted_iota(jnp.int32, (natom, natom), 0)
    col = lax.broadcasted_iota(jnp.int32, (natom, natom), 1)
    offs = jnp.sum(jnp.where(col < row, cnt, 0.0), axis=1, keepdims=True)
    own = jnp.sum(jnp.where(col == row, cnt, 0.0), axis=1, keepdims=True)
    q = q_ref[...]
    q_hi = q.astype(BF16)
    rest = q - q_hi.astype(F32)
    q_mid = rest.astype(BF16)
    q_parts[0] = q_hi
    q_parts[1] = q_mid
    q_parts[2] = (rest - q_mid.astype(F32)).astype(BF16)
    lanes = 256
    nd = qd.shape[0]

    def diagonals(c, _):
        ids = (c * lanes + lax.broadcasted_iota(jnp.int32, (natom, lanes), 1)).astype(F32)
        owns = (offs <= ids) & (ids < offs + own)
        pos = jnp.sum(jnp.where(owns, ids - offs, 0.0), axis=0, keepdims=True)
        count = jnp.sum(jnp.where(owns, jnp.broadcast_to(own, owns.shape), 0.0), axis=0, keepdims=True)
        pick = jnp.where(owns, 1.0, 0.0).astype(BF16)
        flat = jnp.dot(q_parts[0], pick, preferred_element_type=F32)
        flat += jnp.dot(q_parts[1], pick, preferred_element_type=F32)
        flat += jnp.dot(q_parts[2], pick, preferred_element_type=F32)
        q_row = jnp.zeros((mp, lanes), F32)
        for i in range(maxp):
            q_row += jnp.where(pos == float(i), flat[i * mp : (i + 1) * mp], 0.0)
        at = pos + lax.broadcasted_iota(jnp.int32, (nd, lanes), 0).astype(F32) - float(maxp - 1)
        entries = jnp.zeros((nd, lanes), F32)
        for j in range(maxp):
            entries += jnp.where(at == float(j), q_row[j : j + 1], 0.0)
        qd[:, aligned(c, lanes)] = jnp.where(at < count, entries, 0.0)
        return 0

    lax.fori_loop(0, p_size // lanes, diagonals, 0)

    trial_copy.wait()

    def turn(k, _):
        trial_t[:, aligned(k, sw)] = trial_v[aligned(k, sw), :].T
        return 0

    lax.fori_loop(0, s_chunks, turn, 0)

    pl.semaphore_wait(barrier, outer + 2)

    def inner1(c, d):
        at = pl.ds(c * bw, bw)
        return pltpu.make_async_remote_copy(
            src_ref=proj.at[aligned(meant[d], outer * r1), at],
            dst_ref=in1.at[d, :, at],
            send_sem=send1.at[c, d],
            recv_sem=recv1.at[c, d],
            **reach(z, hop[d]),
        )

    def outer1(c, e):
        at = pl.ds(c * bw, bw)
        return pltpu.make_async_remote_copy(
            src_ref=mid1.at[aligned(far(e), r1), at],
            dst_ref=end1.at[e, :, at],
            send_sem=send1b.at[c, e],
            recv_sem=recv1b.at[c, e],
            **reach(far(e), w),
        )

    def relay1(c):
        at = pl.ds(c * bw, bw)
        inner1(c, 3).wait()
        proj[aligned(last, outer * r1), at] += in1[3, :, at]
        inner1(c, 2).start()

    def middle1(c):
        at = pl.ds(c * bw, bw)
        total = proj[aligned(w, outer * r1), at]
        for d in (1, 2):
            inner1(c, d).wait()
            total += in1[d, :, at]
        mid1[:, at] = total
        for e in range(1, outer):
            outer1(c, e).start()

    for c in range(beta_chunks):
        beta_copy(c).wait()
        at = pl.ds(c * bw, bw)
        proj[:, at] = jnp.dot(trial_t[...], beta_v[:, at], preferred_element_type=F32)
        inner1(c, 3).start()
        inner1(c, 1).start()
        if c > 0:
            relay1(c - 1)
        if c > 1:
            middle1(c - 2)
    relay1(beta_chunks - 1)
    middle1(beta_chunks - 2)
    middle1(beta_chunks - 1)

    for c in range(beta_chunks):
        for e in range(1, outer):
            outer1(c, e).wait()
    x = mid1[aligned(z, r1), :]
    for e in range(1, outer):
        x += end1[e]
    acc = jnp.zeros_like(x)
    for d in range(2 * maxp - 1):
        shift = (maxp - 1 - d) % p_size
        moved = x if shift == 0 else pltpu.roll(x, shift, axis=1)
        acc += qd[d : d + 1, :] * moved
    mine = w * outer + z
    wall[aligned(mine, r1), :] = acc

    def outer2(e):
        return pltpu.make_async_remote_copy(
            src_ref=wall.at[aligned(mine, r1), :],
            dst_ref=wall.at[aligned(mine, r1), :],
            send_sem=send2.at[e],
            recv_sem=recv2.at[e],
            **reach(far(e), w),
        )

    def inner2(e, d):
        block = (via if d == 3 else w) * outer + lax.rem(z + outer - e, outer)
        return pltpu.make_async_remote_copy(
            src_ref=wall.at[aligned(block, r1), :],
            dst_ref=wall.at[aligned(block, r1), :],
            send_sem=send2b.at[e, d],
            recv_sem=recv2b.at[e, d],
            **reach(z, via if d == 1 else last),
        )

    for e in range(1, outer):
        outer2(e).start()
    for e in range(outer):
        if e:
            outer2(e).wait()
        for d in (1, 2):
            inner2(e, d).start()
        if e:
            inner2(e - 1, 1).wait()
            inner2(e - 1, 3).start()
    inner2(outer - 1, 1).wait()
    inner2(outer - 1, 3).start()
    for e in range(outer):
        for d in (2, 3):
            inner2(e, d).wait()
    hi, lo = split2(wall[...])
    whl[:cols, :] = hi
    whl[cols:, :] = lo

    base = band * (2 * cols)

    def exchange(k):
        at = (pl.ds(pl.multiple_of(base, 2 * cols), 2 * cols), aligned(k, sw))
        return pltpu.make_async_remote_copy(
            src_ref=s_buf.at[at],
            dst_ref=s_buf.at[at],
            send_sem=xs.at[k],
            recv_sem=xr.at[k],
            device_id=(me, 1 - band),
            device_id_type=MESH,
        )

    def lift(k, _):
        both = lax.dot_general(
            whl[...], beta_v[aligned(k, sw), :], (((1,), (1,)), ((), ())), preferred_element_type=F32
        )
        s = both[:cols] + both[cols:] + trial_t[:, aligned(k, sw)].astype(F32)
        s_hi, s_lo = split2(s)
        s_buf[pl.ds(pl.multiple_of(base, 2 * cols), cols), aligned(k, sw)] = s_hi
        s_buf[pl.ds(pl.multiple_of(base + cols, cols), cols), aligned(k, sw)] = s_lo
        exchange(k).start()
        return 0

    lax.fori_loop(0, s_chunks, lift, 0)

    def wait_x(k, _):
        exchange(k).wait()
        return 0

    lax.fori_loop(0, s_chunks, wait_x, 0)

    def inner3(c, d):
        return pltpu.make_async_remote_copy(
            src_ref=fin.at[:, meant[d], :, aligned(c, pw)],
            dst_ref=in3.at[d, :, :, aligned(c, pw)],
            send_sem=send3.at[c, d],
            recv_sem=recv3.at[c, d],
            **reach(z, hop[d]),
        )

    def outer3(c, e):
        return pltpu.make_async_remote_copy(
            src_ref=mid3.at[far(e), :, aligned(c, pw)],
            dst_ref=end3.at[e, :, aligned(c, pw)],
            send_sem=send3b.at[c, e],
            recv_sem=recv3b.at[c, e],
            **reach(far(e), w),
        )

    def relay3(c):
        inner3(c, 3).wait()
        for to in range(outer):
            fin[to, last, :, aligned(c, pw)] += in3[3, to, :, aligned(c, pw)]
        inner3(c, 2).start()

    def middle3(c):
        for d in (1, 2):
            inner3(c, d).wait()
        for to in range(outer):
            total = fin[to, w, :, aligned(c, pw)]
            for d in (1, 2):
                total += in3[d, to, :, aligned(c, pw)]
            mid3[to, :, aligned(c, pw)] = total
        for e in range(1, outer):
            outer3(c, e).start()

    for c in range(psi_chunks):
        psi_copy(c).wait()

    def share(c):
        f = jnp.dot(s_buf[...], psi_v[:, aligned(c, pw)], preferred_element_type=F32)
        for b in range(2):
            at = 2 * b * cols
            whole = f[at : at + cols] + f[at + cols : at + 2 * cols]
            fin[b * half : (b + 1) * half, :, :, aligned(c, pw)] = whole.reshape(
                half, inner, r2, pw
            )
        inner3(c, 3).start()
        inner3(c, 1).start()

    half = outer // 2
    for c in range(psi_chunks):
        share(c)
        if c > 0:
            relay3(c - 1)
        if c > 1:
            middle3(c - 2)
    relay3(psi_chunks - 1)
    middle3(psi_chunks - 2)
    middle3(psi_chunks - 1)

    for c in range(psi_chunks):
        total = mid3[z, :, aligned(c, pw)]
        for e in range(1, outer):
            outer3(c, e).wait()
            total += end3[e, :, aligned(c, pw)]
        out_ref[:, aligned(c, pw)] = total


def fused(n, inner, blk, psi, trial, beta, q_blocks, atom_counts):
    g, cols = trial.shape
    nbands = psi.shape[1]
    p_size = beta.shape[1]
    natom, maxp = q_blocks.shape[:2]
    mp = -(-maxp // 8) * 8
    nd = -(-(2 * maxp - 1) // 8) * 8
    r1, r2 = cols // n, blk // n
    outer = n // inner
    beta_chunks, psi_chunks, s_chunks = 3, 4, 8
    q_flat = jnp.pad(q_blocks, ((0, 0), (0, 0), (0, mp - maxp)))
    q_flat = q_flat.transpose(1, 2, 0).reshape(maxp * mp, natom)
    dma = pltpu.SemaphoreType.DMA
    out = pl.pallas_call(
        functools.partial(kernel, n, inner, maxp),
        out_shape=jax.ShapeDtypeStruct((r2, nbands), F32),
        in_specs=[pl.BlockSpec(memory_space=pl.ANY)] * 3
        + [pl.BlockSpec(memory_space=pltpu.VMEM)] * 2,
        out_specs=pl.BlockSpec(memory_space=pltpu.VMEM),
        scratch_shapes=[
            pltpu.VMEM((g, nbands), BF16),
            pltpu.VMEM((g, p_size), BF16),
            pltpu.VMEM((g, cols), BF16),
            pltpu.VMEM((cols, g), BF16),
            pltpu.VMEM((3, maxp * mp, natom), BF16),
            pltpu.VMEM((nd, p_size), F32),
            pltpu.VMEM((cols, p_size), F32),
            pltpu.VMEM((inner, outer * r1, p_size), F32),
            pltpu.VMEM((outer * r1, p_size), F32),
            pltpu.VMEM((outer, r1, p_size), F32),
            pltpu.VMEM((cols, p_size), F32),
            pltpu.VMEM((2 * cols, p_size), BF16),
            pltpu.VMEM((4 * cols, g), BF16),
            pltpu.VMEM((outer, inner, r2, nbands), F32),
            pltpu.VMEM((inner, outer, r2, nbands), F32),
            pltpu.VMEM((outer, r2, nbands), F32),
            pltpu.VMEM((outer, r2, nbands), F32),
            dma,
            dma((beta_chunks,)),
            dma((psi_chunks,)),
            dma((beta_chunks, inner)),
            dma((beta_chunks, inner)),
            dma((beta_chunks, outer)),
            dma((beta_chunks, outer)),
            dma((outer,)),
            dma((outer,)),
            dma((outer, inner)),
            dma((outer, inner)),
            dma((s_chunks,)),
            dma((s_chunks,)),
            dma((psi_chunks, inner)),
            dma((psi_chunks, inner)),
            dma((psi_chunks, outer)),
            dma((psi_chunks, outer)),
        ],
        compiler_params=pltpu.CompilerParams(
            collective_id=0, has_side_effects=True, vmem_limit_bytes=60 * 1024 * 1024
        ),
    )(psi, trial, beta, q_flat, atom_counts.reshape(1, natom))
    return out.T


def q_dense(atom_counts, q_blocks, p_size):
    offsets = jnp.cumsum(atom_counts, dtype=jnp.int32) - atom_counts
    natom, maxp = q_blocks.shape[:2]
    ids = jnp.arange(p_size, dtype=jnp.int32)
    owns = (offsets[None, :] <= ids[:, None]) & (ids[:, None] < (offsets + atom_counts)[None, :])
    pos = jnp.sum(jnp.where(owns, ids[:, None] - offsets[None, :], 0), axis=1)
    atom = jnp.sum(jnp.where(owns, jnp.arange(natom, dtype=jnp.int32)[None, :], 0), axis=1)
    flat = jnp.dot(owns.astype(F32), q_blocks.reshape(natom, maxp * maxp), precision=precise)
    place = pos[:, None] == jnp.arange(maxp, dtype=jnp.int32)[None, :]
    rows = jnp.sum(jnp.where(place[:, :, None], flat.reshape(p_size, maxp, maxp), 0.0), axis=1)
    entries = jnp.dot(rows, place.astype(F32).T, precision=precise)
    return jnp.where(atom[:, None] == atom[None, :], entries, 0.0)


def general(psi, trial, beta, q_blocks, atom_counts):
    own = lax.psum(contract(beta, trial), "ga")
    weighted = jnp.dot(q_dense(atom_counts, q_blocks, beta.shape[1]), own, precision=precise)
    w_hi, w_lo = split2(weighted)
    both = jnp.dot(beta, jnp.concatenate([w_hi, w_lo], axis=1), preferred_element_type=F32)
    cols = trial.shape[1]
    s = both[:, :cols] + both[:, cols:] + trial.astype(F32)
    s_hi, s_lo = split2(lax.all_gather(s, "band", axis=1, tiled=True))
    part = contract(psi, s_hi) + contract(psi, s_lo)
    return lax.psum_scatter(part, "ga", scatter_dimension=1, tiled=True)


def solution(mesh):
    n, bands = mesh.shape["ga"], mesh.shape["band"]
    inner = 4

    def shards(psi, trial, beta, q_blocks, atom_counts):
        g, cols = trial.shape
        blk = cols * bands
        fits = (
            bands == 2
            and n % (2 * inner) == 0
            and cols % 128 == 0
            and cols % (8 * n) == 0
            and blk % (8 * n) == 0
            and g % 4096 == 0
            and beta.shape[1] % 768 == 0
            and psi.shape[1] % 512 == 0
            and q_blocks.shape[0] % 128 == 0
        )
        if fits:
            return fused(n, inner, blk, psi, trial, beta, q_blocks, atom_counts)
        return general(psi, trial, beta, q_blocks, atom_counts)

    in_specs = (P("ga", "band"), P("ga", "band"), P("ga", None), P(), P())
    out_specs = P("band", "ga")
    return jax.shard_map(shards, mesh=mesh, in_specs=in_specs, out_specs=out_specs, check_vma=False)
```
